256 devices in a mesh: param: 128 (over z, x, y), sensor: 2 (over core).
Axes of the slice: x: 4, y: 4, z: 8, core: 2. Of those that a mesh axis runs over, the one named last changes fastest.
Arguments:
- data: float32 [16, 512, 420], P(None, ('sensor', 'param')), may hold values from -6 to 6
- spectra: float32 [2, 512, 512, 421], P(None, 'sensor', 'param'), may hold values from -2 to 2
Outputs:
- gradient: float32 [16, 512, 420], P(None, 'param')
- rms: float32 [16], replicated
The draws below stay inside these ranges and needn't reach their ends.
All inputs are finite; a program needn't handle non-finite values.
Results may differ from the reference program's by a relative error of at most 0.0003.
Values sent between devices are 32-bit elements; how exact they have to be, the bound alone decides.
No kernel may reach another device: no remote copies, remote signals or barrier semaphores. Data moves between devices by JAX's collectives and lax.ppermute only.
A program may use at most 128 MiB of HBM per device.

```python
import math
import jax
import jax.numpy as jnp
from jax import lax

SENSORS = 512
NT = 420
NF = 421
P_DEV = 4
NRHS = 16
PARAMS = 512
N_PARAM = 128


def draw_spectra(key, part):
    first = jax.random.fold_in(key, 0)
    shape = (2, SENSORS, PARAMS, NF)
    ramp = 1.0 + jnp.arange(PARAMS, dtype=jnp.float32) / max(PARAMS - 1, 1)
    base = jnp.clip(jax.random.normal(first, shape, jnp.float32), -6.0, 6.0)
    base = base * ramp[None, None, :, None]
    return jnp.clip(base / math.sqrt(SENSORS), -2.0, 2.0)


def shard_levels(rng, dims, cuts, smallest, largest):
    gain = 1.0
    for dim, blocks in cuts:
        heights = jax.random.uniform(jax.random.fold_in(jax.random.fold_in(rng, 6), dim), (blocks,), jnp.float32, smallest / len(cuts), largest / len(cuts))
        gain = gain * jnp.repeat(jnp.exp(heights), dims[dim] // blocks).reshape((-1,) + (1,) * (len(dims) - 1 - dim))
    return gain


def gaussian(rng, shape, scale, limit, shards=(), kind=jnp.bfloat16):
    values = jax.random.normal(rng, shape, jnp.float32) * scale
    if len(shards) > 0:
        values = shard_levels(rng, shape, shards, -0.22, 0.18) * values
    return jnp.clip(values, min=-limit, max=limit).astype(kind)


def setup_inputs(seed: int = 0) -> dict:
    seeds = jax.random.split(jax.random.key(seed), 3)
    data = gaussian(seeds[0], (NRHS, SENSORS, NT), 1.0, 6.0, ((1, 256),), jnp.float32)
    spectra = draw_spectra(jax.random.fold_in(seeds[2], 71), 0)
    return dict(data=data, spectra=spectra)


def reference(data, spectra):
    data_hat = jnp.fft.rfft(data, n=2 * NT, axis=-1)
    real_part = jnp.real(data_hat).astype(jnp.float32)
    imag_part = jnp.imag(data_hat).astype(jnp.float32)

    def one_block(index):
        start = (index * P_DEV).astype(jnp.int32)
        kernel = lax.dynamic_slice_in_dim(spectra, start, P_DEV, 2)
        kernel_re = kernel[0]
        kernel_im = kernel[1]
        hi = lax.Precision.HIGHEST
        out_re = jnp.einsum('spf,rsf->rpf', kernel_re, real_part, precision=hi) + jnp.einsum('spf,rsf->rpf', kernel_im, imag_part, precision=hi)
        out_im = jnp.einsum('spf,rsf->rpf', kernel_re, imag_part, precision=hi) - jnp.einsum('spf,rsf->rpf', kernel_im, real_part, precision=hi)
        return (out_re, out_im)
    blocks_re, blocks_im = lax.map(one_block, jnp.arange(N_PARAM, dtype=jnp.int32))
    whole_re = jnp.transpose(blocks_re, (1, 0, 2, 3)).reshape(data.shape[0], PARAMS, NF)
    whole_im = jnp.transpose(blocks_im, (1, 0, 2, 3)).reshape(data.shape[0], PARAMS, NF)
    field = jnp.fft.irfft(whole_re + 1j * whole_im, n=2 * NT, axis=-1)[..., :NT].astype(jnp.float32)
    rms = jnp.sqrt(lax.optimization_barrier(jnp.mean(field * field, axis=(1, 2))) + 1e-06)
    return (field / rms[:, None, None], rms)
```

```python
import functools
import math

import jax
import jax.numpy as jnp
from jax import lax
from jax.experimental import pallas as pl
from jax.experimental.pallas import tpu as pltpu
from jax.sharding import Mesh
from jax.sharding import PartitionSpec as P

Z, X, Y, C = "param_0", "param_1", "param_2", "sensor"
PARAM = (Z, X, Y)
STEPS = 420
HALF = STEPS // 2
LENGTH = 2 * STEPS
FREQS = STEPS + 1
ROWS = 56
RING = (0, -1, 1, 2)


def shift(array, axis, step):
    n = lax.axis_size(axis)
    return lax.ppermute(array, axis, [(i, (i + step) % n) for i in range(n)])


def swap(array, axis):
    n = lax.axis_size(axis)
    return lax.ppermute(array, axis, [(i, i ^ 1) for i in range(n)])


def ring_of_four(array, axis):
    left = shift(array, axis, 1)
    right = shift(array, axis, -1)
    half = array.shape[0] // 2
    return [array, left, right, shift(left[:half], axis, 1), shift(right[half:], axis, -1)]


def lane_freq(lane):
    odd = lane // 256
    late = lane % 256 // 128
    g = lane % 128 + late * (83 - odd)
    return 2 * g + odd, (late == 0) | (g >= 128)


def forward_tables():
    row = lax.broadcasted_iota(jnp.int32, (256, 512), 0)
    col = lax.broadcasted_iota(jnp.int32, (256, 512), 1)
    imag = col >= 256
    out = []
    for kind in (0, 1):
        if kind == 0:
            t = row
            used = row < 211
            lane = jnp.where(imag, col, col)
        else:
            t = jnp.where(row < 128, row, jnp.where(row < 192, row + 45, row - 64))
            used = (row < 128) | ((row >= 147) & (row < 165)) | (row >= 192)
            lane = jnp.where(imag, col - 256, col + 256)
        freq, _ = lane_freq(lane)
        phase = 2.0 * math.pi / LENGTH * (t * freq % LENGTH).astype(jnp.float32)
        table = jnp.where(used, jnp.where(imag, -jnp.sin(phase), jnp.cos(phase)), 0.0)
        out.append(table)
    return out


def backward_table():
    row = lax.broadcasted_iota(jnp.int32, (1024, 512), 0)
    t = lax.broadcasted_iota(jnp.int32, (1024, 512), 1)
    freq, used = lane_freq(row % 512)
    imag = row >= 512
    phase = 2.0 * math.pi / LENGTH * (t * freq % LENGTH).astype(jnp.float32)
    edge = (freq == 0) | (freq == STEPS)
    weight = jnp.where(edge, jnp.where(imag, 0.0, 1.0), 2.0) / LENGTH
    weight = jnp.where(used & (t < STEPS), weight, 0.0)
    return weight * jnp.where(imag, -jnp.sin(phase), jnp.cos(phase))


def two_parts(table):
    high = lax.reduce_precision(table, 8, 7)
    return high.astype(jnp.bfloat16), (table - high).astype(jnp.bfloat16)


def pack_kernel(data_ref, out_ref):
    row = lax.broadcasted_iota(jnp.int32, (STEPS, 512), 0)
    col = lax.broadcasted_iota(jnp.int32, (STEPS, 512), 1)
    lane = col % 64
    is_b = ((col >= 128) & (col < 256)) | ((col >= 320) & (col < 384)) | ((col >= 384) & (lane >= 19))
    t = jnp.where(
        col < 256,
        col % 128,
        jnp.where(col < 384, 128 + lane, jnp.where(lane < 19, 192 + lane, 173 + lane)),
    )
    used = (col < 384) | ((col < 448) & (lane < 37))
    mirror = (row == STEPS - t) & (t != HALF)
    value = jnp.where(row == t, 1.0, jnp.where(mirror, jnp.where(is_b, -1.0, 1.0), 0.0))
    fold = jnp.where(used, value, 0.0)
    packed = []
    for j in range(2):
        series = data_ref[:, j, :]
        packed.append(
            jnp.dot(series, fold, precision=lax.Precision.HIGHEST, preferred_element_type=jnp.float32)
        )
    lanes = lax.broadcasted_iota(jnp.int32, (16, 128), 1)
    tail0 = packed[0][:, 384:512]
    tail1 = pltpu.roll(packed[1][:, 384:512], 64, 1)
    tiles = []
    for start in (0, 128, 256):
        for j in range(2):
            tiles.append(packed[j][:, start : start + 128])
    tiles.append(jnp.where(lanes < 64, tail0, tail1))
    for half in range(2):
        for g, tile in enumerate(tiles):
            piece = tile[half * 8 : half * 8 + 8, :]
            for to in range(out_ref.shape[0]):
                out_ref[to, half, g * 8 : g * 8 + 8, :] = piece


def pack(data):
    return pl.pallas_call(
        pack_kernel,
        out_shape=jax.ShapeDtypeStruct((8, 2, ROWS, 128), jnp.float32),
        in_specs=[pl.BlockSpec(memory_space=pltpu.VMEM)],
        out_specs=pl.BlockSpec(memory_space=pltpu.VMEM),
        name="pack",
    )(data)


def split_parts(value):
    high = value.astype(jnp.bfloat16)
    return high, (value - high.astype(jnp.float32)).astype(jnp.bfloat16)


def dot3(lhs, rhs):
    (lh, ll), (rh, rl) = lhs, rhs
    dot = functools.partial(jnp.dot, preferred_element_type=jnp.float32)
    return dot(lh, rh) + dot(lh, rl) + dot(ll, rh)


def compute_kernel(place, *refs):
    data_refs = refs[:10]
    own_ref, other_ref, wa_h, wa_l, wb_h, wb_l, wi_h, wi_l, out_ref = refs[10:19]
    kt, la_h, la_l, lb_h, lb_l, xa, xb, spec = refs[19:]
    low = lax.broadcasted_iota(jnp.int32, (8, 128), 1) < 64

    for which, ref in enumerate((own_ref, other_ref)):

        def turn(p, carry, which=which, ref=ref):
            for odd in range(2):
                for late in range(2):
                    first = 2 * late * (83 - odd) + odd
                    lanes = slice((odd * 2 + late) * 128, (odd * 2 + late) * 128 + 128)
                    re = ref[pl.ds(first * 4 + p, 128, stride=8), :].T
                    im = ref[pl.ds((FREQS + first) * 4 + p, 128, stride=8), :].T
                    kt[which, p, :, :, lanes] = re.reshape(16, 8, 128)
                    kt[which, 4 + p, :, :, lanes] = im.reshape(16, 8, 128)
                    kt[which, 8 + p, :, :, lanes] = (re - im).reshape(16, 8, 128)
            return carry

        lax.fori_loop(0, 4, turn, 0)

    for half in range(2):
        outer = 1 if half == 0 else 0
        inner = 1 - outer
        parts = data_refs[half * 5 : half * 5 + 5]
        for n, ref in enumerate(parts):
            blocks = range(4) if n < 3 else (range(2) if n == 3 else range(2, 4))
            for at, block in enumerate(blocks):
                out_at = lax.rem(place[outer] + (RING[min(n, 3)] + 4), 4)
                in_at = lax.rem(place[inner] + (RING[block] + 4), 4)
                x_at, y_at = (in_at, out_at) if half == 0 else (out_at, in_at)

                def unpack(z, carry, ref=ref, at=at, half=half, x_at=x_at, y_at=y_at):
                    base = at * 4 * ROWS + z * ROWS
                    tile = lambda g: ref[pl.ds(pl.multiple_of(base + g * 8, 8), 8), :]
                    tail = tile(6)
                    turned = pltpu.roll(tail, 64, 1)
                    a = []
                    b = []
                    for j in range(2):
                        c = tile(4 + j)
                        up, down = (turned, tail) if j == 0 else (tail, turned)
                        a.append(jnp.concatenate([tile(j), jnp.where(low, c, up)], axis=1))
                        b.append(jnp.concatenate([tile(2 + j), jnp.where(low, down, c)], axis=1))
                    pair = z * 16 + x_at * 4 + y_at
                    la_h[half, pair], la_l[half, pair] = split_parts(jnp.concatenate(a, axis=0))
                    lb_h[half, pair], lb_l[half, pair] = split_parts(jnp.concatenate(b, axis=0))
                    return carry

                lax.fori_loop(0, 4, unpack, 0)

    for half in range(2):

        def transform(m, carry, half=half):
            take = lambda ref: ref[half, pl.ds(m * 16, 16)].reshape(256, 256)
            to = pl.ds(pl.multiple_of(half * 1024 + m * 256, 256), 256)
            xa[to, :] = dot3((take(la_h), take(la_l)), (wa_h[...], wa_l[...]))
            xb[to, :] = dot3((take(lb_h), take(lb_l)), (wb_h[...], wb_l[...]))
            return carry

        lax.fori_loop(0, 4, transform, 0)

    for which in range(2):
        for odd in range(2):
            for late in range(2):
                here = slice(late * 128, late * 128 + 128)
                there = slice(256 + late * 128, 256 + late * 128 + 128)
                re_ref, im_ref = (xa, xb) if odd == 0 else (xb, xa)
                lanes = slice((odd * 2 + late) * 128, (odd * 2 + late) * 128 + 128)

                def add(s8, acc, which=which, here=here, there=there, re_ref=re_ref, im_ref=im_ref, lanes=lanes):
                    acc = list(acc)
                    for i in range(8):
                        s = s8 * 8 + i
                        xs = []
                        for half in range(2):
                            rows = pl.ds(pl.multiple_of(half * 1024 + s * 8, 8), 8)
                            re = re_ref[rows, here]
                            im = im_ref[rows, there]
                            xs.append((re, im, re + im))
                        for p in range(4):
                            for part in range(3):
                                k = jnp.broadcast_to(kt[which, part * 4 + p, s8, i : i + 1, lanes], (8, 128))
                                for half in range(2):
                                    n = (p * 2 + half) * 3 + part
                                    acc[n] = acc[n] + k * xs[half][part]
                    return tuple(acc)

                zero = jnp.zeros((8, 128), jnp.float32)
                acc = lax.fori_loop(0, 16, add, (zero,) * 24)
                for p in range(4):
                    for half in range(2):
                        one, two, three = acc[(p * 2 + half) * 3 : (p * 2 + half) * 3 + 3]
                        rows = slice(which * 64 + p * 16 + half * 8, which * 64 + p * 16 + half * 8 + 8)
                        spec[rows, lanes] = one + two
                        spec[rows, slice(512 + lanes.start, 512 + lanes.stop)] = three - one + two

    out_ref[...] = dot3(split_parts(spec[...]), (wi_h[...], wi_l[...]))


def compute(place, arrays):
    vmem = pl.BlockSpec(memory_space=pltpu.VMEM)
    bf16 = functools.partial(pltpu.VMEM, dtype=jnp.bfloat16)
    return pl.pallas_call(
        compute_kernel,
        out_shape=jax.ShapeDtypeStruct((128, 512), jnp.float32),
        in_specs=[pl.BlockSpec(memory_space=pltpu.SMEM)] + [vmem] * len(arrays),
        out_specs=vmem,
        scratch_shapes=[pltpu.VMEM((2, 12, 16, 8, 512), jnp.float32)]
        + [pltpu.VMEM((2, 64, 16, 256), jnp.bfloat16)] * 4
        + [pltpu.VMEM((2048, 512), jnp.float32)] * 2
        + [pltpu.VMEM((128, 1024), jnp.float32)],
        compiler_params=pltpu.CompilerParams(vmem_limit_bytes=60 << 20),
        cost_estimate=pl.CostEstimate(flops=20_000_000_000, bytes_accessed=10_000_000, transcendentals=0),
        name="adjoint",
    )(place, *arrays)


def body(data, spectra):
    odd = lax.axis_index(Z) % 2
    place = jnp.stack([lax.axis_index(X), lax.axis_index(Y)]).astype(jnp.int32)
    kernel = spectra.transpose(0, 3, 2, 1)
    own = lax.dynamic_slice_in_dim(kernel, odd * 128, 128, 3).reshape(-1, 128)
    given = lax.dynamic_slice_in_dim(kernel, (1 - odd) * 128, 128, 3).reshape(-1, 128)
    other = swap(given, Z)

    packed = pack(data)
    column = lax.all_to_all(packed, Z, split_axis=0, concat_axis=0, tiled=True)
    column = lax.dynamic_slice_in_dim(column, odd * 4, 4, 0)
    blocks = []
    for half, axes in enumerate(((X, Y), (Y, X))):
        ring = ring_of_four(column[:, half].reshape(4 * ROWS, 128), axes[0])
        blocks += ring_of_four(jnp.concatenate(ring, axis=0), axes[1])

    tables = [part for table in (*forward_tables(), backward_table()) for part in two_parts(table)]
    fields = compute(place, [*blocks, own, other, *tables])
    field = fields[:64] + swap(fields[64:], Z)
    field = field + swap(field, C)
    field = field[:, :STEPS].reshape(4, 16, STEPS)
    squares = jnp.sum(field * field, axis=(0, 2))
    everyone = jnp.broadcast_to(squares, (128, 1, 16))
    total = lax.all_to_all(everyone, PARAM, split_axis=0, concat_axis=0, tiled=True).sum(axis=(0, 1))
    scale = jnp.sqrt(total / (4 * 128 * STEPS) + 1e-06)
    return (field / scale[None, :, None]).transpose(1, 0, 2), scale


def solution(mesh):
    split = Mesh(mesh.devices.reshape(8, 4, 4, mesh.shape["sensor"]), (*PARAM, C))
    placed = (P(None, (C, *PARAM), None), P(None, C, PARAM, None))
    return jax.shard_map(
        body, mesh=split, in_specs=placed, out_specs=(P(None, PARAM, None), P()), check_vma=False
    )
```

```python
import functools
import math

import jax
import jax.numpy as jnp
from jax import lax
from jax.experimental import pallas as pl
from jax.experimental.pallas import tpu as pltpu
from jax.sharding import Mesh
from jax.sharding import PartitionSpec as P

Z, X, Y, C = "param_0", "param_1", "param_2", "sensor"
PARAM = (Z, X, Y)
STEPS = 420
HALF = STEPS // 2
LENGTH = 2 * STEPS
FREQS = STEPS + 1
ROWS = 56
RING = (0, -1, 1, 2)


def shift(array, axis, step):
    n = lax.axis_size(axis)
    return lax.ppermute(array, axis, [(i, (i + step) % n) for i in range(n)])


def swap(array, axis):
    n = lax.axis_size(axis)
    return lax.ppermute(array, axis, [(i, i ^ 1) for i in range(n)])


def gather_four(array, axis):
    parts = [array, shift(array, axis, 1), shift(array, axis, -1), shift(array, axis, 2)]
    return jnp.concatenate(parts, axis=0)


def ring_of_four(array, axis):
    left = shift(array, axis, 1)
    right = shift(array, axis, -1)
    half = array.shape[0] // 2
    far = (shift(left[:half], axis, 1), shift(right[half:], axis, -1))
    return (array,), (left, right), far


def lane_freq(lane):
    odd = lane // 256
    late = lane % 256 // 128
    g = lane % 128 + late * (83 - odd)
    return 2 * g + odd, (late == 0) | (g >= 128)


def cosine(product):
    turn = product - LENGTH * jnp.floor(product * (1.0 / LENGTH))
    v = jnp.abs(jnp.where(turn > STEPS, turn - LENGTH, turn)) - HALF
    x = v * (math.pi / STEPS)
    y = x * x
    total = 1.0 / math.factorial(11)
    for n in (9, 7, 5, 3, 1):
        total = 1.0 / math.factorial(n) - y * total
    return -x * total


def tables_kernel(wa_h, wa_l, wb_h, wb_l, wi_h, wi_l):
    quarter = LENGTH // 4
    col = lax.broadcasted_iota(jnp.int32, (16, 512), 1)
    row16 = lax.broadcasted_iota(jnp.int32, (16, 512), 0)
    imag = (col >= 256).astype(jnp.float32)
    freq_a = lane_freq(col)[0].astype(jnp.float32)
    freq_b = lane_freq(jnp.where(col >= 256, col - 256, col + 256))[0].astype(jnp.float32)

    def forward(i, carry):
        row = row16 + i * 16
        rows = pl.ds(pl.multiple_of(i * 16, 16), 16)
        table = jnp.where(row < 211, cosine(row.astype(jnp.float32) * freq_a + quarter * imag), 0.0)
        wa_h[rows, :], wa_l[rows, :] = split_parts(table)
        t = jnp.where(row < 128, row, jnp.where(row < 192, row + 45, row - 64))
        used = (row < 128) | ((row >= 147) & (row < 165)) | (row >= 192)
        table = jnp.where(used, cosine(t.astype(jnp.float32) * freq_b + quarter * imag), 0.0)
        wb_h[rows, :], wb_l[rows, :] = split_parts(table)
        return carry

    lax.fori_loop(0, 16, forward, 0)
    time = col.astype(jnp.float32)

    def backward(i, carry):
        row = row16 + i * 16
        rows = pl.ds(pl.multiple_of(i * 16, 16), 16)
        freq, used = lane_freq(row % 512)
        edge = (freq == 0) | (freq == STEPS)
        sine = row >= 512
        weight = jnp.where(edge, jnp.where(sine, 0.0, 1.0), 2.0) * (1.0 / LENGTH)
        weight = jnp.where(used & (col < STEPS), weight, 0.0)
        shift = jnp.where(sine, float(quarter), 0.0)
        table = weight * cosine(time * freq.astype(jnp.float32) + shift)
        wi_h[rows, :], wi_l[rows, :] = split_parts(table)
        return carry

    lax.fori_loop(0, 64, backward, 0)


def make_tables():
    small = jax.ShapeDtypeStruct((256, 512), jnp.bfloat16)
    large = jax.ShapeDtypeStruct((1024, 512), jnp.bfloat16)
    return pl.pallas_call(
        tables_kernel,
        out_shape=(small,) * 4 + (large,) * 2,
        out_specs=(pl.BlockSpec(memory_space=pltpu.VMEM),) * 6,
        cost_estimate=pl.CostEstimate(flops=30_000_000, bytes_accessed=3_000_000, transcendentals=0),
        compiler_params=pltpu.CompilerParams(vmem_limit_bytes=8 << 20),
        name="tables",
    )()


def pack_kernel(data_ref, out_ref):
    row = lax.broadcasted_iota(jnp.int32, (STEPS, 512), 0)
    col = lax.broadcasted_iota(jnp.int32, (STEPS, 512), 1)
    lane = col % 64
    is_b = ((col >= 128) & (col < 256)) | ((col >= 320) & (col < 384)) | ((col >= 384) & (lane >= 19))
    t = jnp.where(
        col < 256,
        col % 128,
        jnp.where(col < 384, 128 + lane, jnp.where(lane < 19, 192 + lane, 173 + lane)),
    )
    used = (col < 384) | ((col < 448) & (lane < 37))
    mirror = (row == STEPS - t) & (t != HALF)
    value = jnp.where(row == t, 1.0, jnp.where(mirror, jnp.where(is_b, -1.0, 1.0), 0.0))
    fold = jnp.where(used, value, 0.0)
    packed = []
    for j in range(2):
        series = data_ref[:, j, :]
        packed.append(
            jnp.dot(series, fold, precision=lax.Precision.HIGHEST, preferred_element_type=jnp.float32)
        )
    lanes = lax.broadcasted_iota(jnp.int32, (16, 128), 1)
    tail0 = packed[0][:, 384:512]
    tail1 = pltpu.roll(packed[1][:, 384:512], 64, 1)
    tiles = []
    for start in (0, 128, 256):
        for j in range(2):
            tiles.append(packed[j][:, start : start + 128])
    tiles.append(jnp.where(lanes < 64, tail0, tail1))
    for half in range(2):
        for g, tile in enumerate(tiles):
            piece = tile[half * 8 : half * 8 + 8, :]
            for to in range(out_ref.shape[0]):
                out_ref[to, half, g * 8 : g * 8 + 8, :] = piece


def pack(data):
    return pl.pallas_call(
        pack_kernel,
        out_shape=jax.ShapeDtypeStruct((8, 2, ROWS, 128), jnp.float32),
        in_specs=[pl.BlockSpec(memory_space=pltpu.VMEM)],
        out_specs=pl.BlockSpec(memory_space=pltpu.VMEM),
        compiler_params=pltpu.CompilerParams(vmem_limit_bytes=4 << 20),
        name="pack",
    )(data)


def split_parts(value):
    high = value.astype(jnp.bfloat16)
    return high, (value - high.astype(jnp.float32)).astype(jnp.bfloat16)


def dot3(lhs, rhs):
    (lh, ll), (rh, rl) = lhs, rhs
    dot = functools.partial(jnp.dot, preferred_element_type=jnp.float32)
    return dot(lh, rh) + dot(lh, rl) + dot(ll, rh)


def turn_spectra(y, ref, kt):
    away = lax.rem(8 - 2 * y, 8)

    def turn(p, carry):
        for odd in range(2):
            for late in range(2):
                first = 2 * late * (83 - odd) + odd
                lanes = slice((odd * 2 + late) * 128, (odd * 2 + late) * 128 + 128)
                re = ref[pl.ds(first * 4 + p, 128, stride=8), :].T
                im = ref[pl.ds((FREQS + first) * 4 + p, 128, stride=8), :].T
                for n in range(16):
                    rows = slice(n * 8, n * 8 + 8)
                    re8 = pltpu.roll(re[rows], away, 0)
                    im8 = pltpu.roll(im[rows], away, 0)
                    kt[p, n, :, lanes] = re8
                    kt[4 + p, n, :, lanes] = im8
                    kt[8 + p, n, :, lanes] = re8 - im8
        return carry

    lax.fori_loop(0, 4, turn, 0)


def transform(place, units, tables, lhs, xa, xb):
    wa_h, wa_l, wb_h, wb_l = tables
    la_h, la_l, lb_h, lb_l = lhs
    low = lax.broadcasted_iota(jnp.int32, (8, 128), 1) < 64
    for unit, (half, refs) in enumerate(units):
        for ref, blocks in refs:
            for at, block in enumerate(blocks):
                pos = lax.rem(place[0] + (RING[block] + 4), 4) if half == 0 else RING[block] % 4
                for z in range(4):
                    base = at * 4 * ROWS + z * ROWS
                    tiles = [ref[base + g * 8 : base + g * 8 + 8, :] for g in range(7)]
                    tail = tiles[6]
                    turned = pltpu.roll(tail, 64, 1)
                    a = []
                    b = []
                    for j in range(2):
                        c = tiles[4 + j]
                        up, down = (turned, tail) if j == 0 else (tail, turned)
                        a.append(jnp.concatenate([tiles[j], jnp.where(low, c, up)], axis=1))
                        b.append(jnp.concatenate([tiles[2 + j], jnp.where(low, down, c)], axis=1))
                    pair = z * 4 + pos
                    la_h[unit, pair], la_l[unit, pair] = split_parts(jnp.concatenate(a, axis=0))
                    lb_h[unit, pair], lb_l[unit, pair] = split_parts(jnp.concatenate(b, axis=0))
    for unit in range(len(units)):
        take = lambda ref: ref[unit].reshape(256, 256)
        xa[unit] = dot3((take(la_h), take(la_l)), (wa_h[...], wa_l[...]))
        xb[unit] = dot3((take(lb_h), take(lb_l)), (wb_h[...], wb_l[...]))


def add_sensors(place, sources, kt, spec, base=None):
    for half in range(2):
        for odd in range(2):

            def add(n, acc, xa, xb, unit, hops):
                acc = list(acc)
                re_ref, im_ref = (xa, xb) if odd == 0 else (xb, xa)
                for i in range(8):
                    if half == 0:
                        group = n * 4 + i // 2
                        row = hops % 4 * 2 + i % 2
                    else:
                        group = n * 4 + lax.rem(place[0] + (hops + 4), 4)
                        row = i
                    rows = pl.ds(pl.multiple_of(n * 64 + i * 8, 8), 8)
                    for late in range(2):
                        lanes = slice((odd * 2 + late) * 128, (odd * 2 + late) * 128 + 128)
                        re = re_ref[unit, rows, late * 128 : late * 128 + 128]
                        im = im_ref[unit, rows, 256 + late * 128 : 256 + late * 128 + 128]
                        xs = (re, im, re + im)
                        for p in range(4):
                            for part in range(3):
                                k = jnp.broadcast_to(kt[part * 4 + p, group, row : row + 1, lanes], (8, 128))
                                m = (late * 4 + p) * 3 + part
                                acc[m] = acc[m] + k * xs[part]
                return tuple(acc)

            acc = (jnp.zeros((8, 128), jnp.float32),) * 24
            for of_half, hops, xa, xb, unit in sources:
                if of_half == half:
                    acc = lax.fori_loop(0, 4, functools.partial(add, xa=xa, xb=xb, unit=unit, hops=hops), acc)
            for late in range(2):
                for p in range(4):
                    one, two, three = acc[(late * 4 + p) * 3 : (late * 4 + p) * 3 + 3]
                    rows = slice(p * 16 + half * 8, p * 16 + half * 8 + 8)
                    lanes = slice((odd * 2 + late) * 128, (odd * 2 + late) * 128 + 128)
                    beyond = slice(512 + lanes.start, 512 + lanes.stop)
                    re = one + two
                    im = three - one + two
                    if base is not None:
                        re = re + base[rows, lanes]
                        im = im + base[rows, beyond]
                    spec[rows, lanes] = re
                    spec[rows, beyond] = im


UNITS = {
    "own": ((0, 0), (1, 0)),
    "near": ((0, -1), (0, 1), (1, -1), (1, 1)),
    "far": ((0, 2), (1, 2)),
}


def turn_kernel(place, ref, kt):
    turn_spectra(place[1], ref, kt)


def early_kernel(name, with_base, place, *refs):
    units = UNITS[name]
    data = refs[: len(units)]
    refs = refs[len(units) :]
    tables, refs = refs[:4], refs[4:]
    kt, refs = refs[0], refs[1:]
    base, refs = (refs[0], refs[1:]) if with_base else (None, refs)
    xa, xb, spec = refs[:3]
    transform(place, [(half, [(ref, range(4))]) for (half, _), ref in zip(units, data)], tables, refs[3:], xa, xb)
    add_sensors(place, [(half, hops, xa, xb, n) for n, (half, hops) in enumerate(units)], kt, spec, base)


def late_kernel(place, ref, xa1, xb1, xa2, xb2, kt, spec):
    turn_spectra(place[1], ref, kt)
    sources = [(half, hops, xa1, xb1, n) for n, (half, hops) in enumerate(UNITS["own"])]
    sources += [(half, hops, xa2, xb2, n) for n, (half, hops) in enumerate(UNITS["near"])]
    add_sensors(place, sources, kt, spec)


def last_kernel(place, d0, d1, d2, d3, wa_h, wa_l, wb_h, wb_l, kt_own, kt_other, own, other, wi_h, wi_l, *refs):
    mine, theirs, xa, xb, spec, *lhs = refs
    parts = [(0, [(d0, (0, 1)), (d1, (2, 3))]), (1, [(d2, (0, 1)), (d3, (2, 3))])]
    transform(place, parts, (wa_h, wa_l, wb_h, wb_l), lhs, xa, xb)
    sources = [(half, hops, xa, xb, n) for n, (half, hops) in enumerate(UNITS["far"])]
    add_sensors(place, sources, kt_own, spec.at[0:64], own)
    add_sensors(place, sources, kt_other, spec.at[64:128], other)
    field = dot3(split_parts(spec[...]), (wi_h[...], wi_l[...]))
    mine[...] = field[:64]
    theirs[...] = field[64:]


def call(kernel, operands, outs, scratch, mib, flops):
    vmem = pl.BlockSpec(memory_space=pltpu.VMEM)
    return pl.pallas_call(
        kernel,
        out_shape=outs,
        in_specs=[pl.BlockSpec(memory_space=pltpu.SMEM)] + [vmem] * (len(operands) - 1),
        out_specs=(vmem,) * len(outs) if isinstance(outs, tuple) else vmem,
        scratch_shapes=scratch,
        compiler_params=pltpu.CompilerParams(vmem_limit_bytes=mib << 20),
        cost_estimate=pl.CostEstimate(flops=flops, bytes_accessed=10_000_000, transcendentals=0),
    )(*operands)


def f32(*shape):
    return jax.ShapeDtypeStruct(shape, jnp.float32)


def lhs_scratch(units):
    return [pltpu.VMEM((units, 16, 16, 256), jnp.bfloat16)] * 4


KT = (12, 16, 8, 512)


def early(name, place, data, tables, kt, base):
    units = len(UNITS[name])
    operands = [place, *data, *tables, kt] + ([] if base is None else [base])
    outs = (f32(units, 256, 512), f32(units, 256, 512), f32(64, 1024))
    kernel = functools.partial(early_kernel, name, base is not None)
    return call(kernel, operands, outs, lhs_scratch(units), 14, units * 40_000_000)


def body(data, spectra):
    odd = lax.axis_index(Z) % 2
    place = jnp.stack([lax.axis_index(X), lax.axis_index(Y)]).astype(jnp.int32)
    packed = pack(data)
    kernel = spectra.transpose(0, 3, 2, 1)
    given = lax.dynamic_slice_in_dim(kernel, (1 - odd) * 128, 128, 3).reshape(-1, 128)
    other = swap(given, Z)
    column = lax.all_to_all(packed, Z, split_axis=0, concat_axis=0, tiled=True)
    *tables, wi_h, wi_l = make_tables()
    column = lax.dynamic_slice_in_dim(column, odd * 4, 4, 0)
    own = lax.dynamic_slice_in_dim(kernel, odd * 128, 128, 3).reshape(-1, 128)
    kt_own = call(turn_kernel, [place, own], f32(*KT), [], 12, 40_000_000)
    rings = []
    for half, axes in enumerate(((X, Y), (Y, X))):
        block = gather_four(column[:, half].reshape(4 * ROWS, 128), axes[0])
        rings.append(ring_of_four(block, axes[1]))
    here, near, far = ([*first, *second] for first, second in zip(*rings))
    xa1, xb1, spec1 = early("own", place, here, tables, kt_own, None)
    xa2, xb2, spec2 = early("near", place, near, tables, kt_own, spec1)
    kt_other, spec3 = call(
        late_kernel, [place, other, xa1, xb1, xa2, xb2], (f32(*KT), f32(64, 1024)), [], 14, 150_000_000
    )
    mine, theirs = call(
        last_kernel,
        [place, *far, *tables, kt_own, kt_other, spec2, spec3, wi_h, wi_l],
        (f32(64, 512), f32(64, 512)),
        [pltpu.VMEM((2, 256, 512), jnp.float32)] * 2 + [pltpu.VMEM((128, 1024), jnp.float32)] + lhs_scratch(2),
        14,
        100_000_000,
    )
    field = mine + swap(theirs, Z)
    field = field + swap(field, C)
    field = field[:, :STEPS].reshape(4, 16, STEPS)
    squares = jnp.sum(field * field, axis=(0, 2))
    everyone = jnp.broadcast_to(squares, (128, 1, 16))
    total = lax.all_to_all(everyone, PARAM, split_axis=0, concat_axis=0, tiled=True).sum(axis=(0, 1))
    scale = jnp.sqrt(total / (4 * 128 * STEPS) + 1e-06)
    return (field / scale[None, :, None]).transpose(1, 0, 2), scale


def solution(mesh):
    split = Mesh(mesh.devices.reshape(8, 4, 4, mesh.shape["sensor"]), (*PARAM, C))
    placed = (P(None, (C, *PARAM), None), P(None, C, PARAM, None))
    return jax.shard_map(
        body, mesh=split, in_specs=placed, out_specs=(P(None, PARAM, None), P()), check_vma=False
    )
```
